256 devices in a mesh: ang: 64 (over z_lo, x, y, core), box: 4 (over z_hi).
Axes of the slice: x: 4, y: 4, z: 8 (z_hi: 4, z_lo: 2; z = z_hi * 2 + z_lo), core: 2. Of those that a mesh axis runs over, the one named last changes fastest.
Arguments:
- incoming: float32 [2, 32, 32, 32768], P(None, None, 'box', 'ang'), may hold values from -6 to 6
- own_field: bfloat16 [2, 32, 256, 8192], P(None, None, 'box', 'ang'), may hold values from -6 to 6
- phase_mid: float32 [256, 8192], P('box', 'ang'), may hold values from -3.140625 to 3.140625
- phase_leaf: float32 [2048, 2048], P(('ang', 'box')), may hold values from -3.140625 to 3.140625
- phase_low: float32 [16384, 512], P(('ang', 'box')), may hold values from -3.140625 to 3.140625
- weight_top: float32 [4, 32768], P(None, 'ang'), may hold values from -0.3 to 1
- weight_leaf: float32 [4, 8192], replicated, may hold values from -0.3 to 1
- weight_low: float32 [4, 2048], replicated, may hold values from -0.3 to 1
- offsets: int32 [4], replicated, may hold values from -2 to 2, as said below
- owner: int32 [4, 64], replicated, may hold values from 0 to 63, each once within a row
Outputs:
- lower_field: float32 [2, 32, 16384, 512], P(None, None, ('ang', 'box'))
The draws below stay inside these ranges and needn't reach their ends.
Inputs may be any that keep to these rules, and one draw needn't show every extreme that they name: `offsets`: the first entry is -2 and the last is 2. `owner`: each row is a permutation of the ang indices.
All inputs are finite; a program needn't handle non-finite values.
Results may differ from the reference program's by a relative error of at most 0.0003.
Values sent between devices are 32-bit elements; how exact they have to be, the bound alone decides.
No kernel may reach another device: no remote copies, remote signals or barrier semaphores. Data moves between devices by JAX's collectives and lax.ppermute only.
A program may use at most 64 MiB of HBM per device.

```python
import jax
import jax.numpy as jnp

RHS = 32
K2 = 32768
STENCIL = 4
REACH = 2
RATIO = 4
CHILDREN = 8
K1 = 8192
K0 = 2048
K3 = 512
B1 = 256
B2 = 32
B0 = 2048
B3 = 16384
N_ANG = 64
N_BOX = 4


def draw_offsets(key, part):
    middle_key = jax.random.fold_in(key, 17)
    lowest = jnp.full((1,), -REACH, jnp.int32)
    highest = jnp.full((1,), REACH, jnp.int32)
    middle = jax.random.randint(middle_key, (STENCIL - 2,), -REACH, REACH + 1)
    return jnp.concatenate([lowest, middle.astype(jnp.int32), highest]).astype(jnp.int32)


def block_scale(own_key, dims, shards, least, largest):
    factor_of = 1.0
    for axis_at, parts in shards:
        heights = jax.random.uniform(jax.random.fold_in(jax.random.fold_in(own_key, 6), axis_at), (parts,), jnp.float32, least / len(shards), largest / len(shards))
        factor_of = factor_of * jnp.repeat(jnp.exp(heights), dims[axis_at] // parts).reshape((-1,) + (1,) * (len(dims) - 1 - axis_at))
    return factor_of


def bell_draw(rng, extent, width, bound, pieces=(), held_as=jnp.bfloat16):
    result = width * jax.random.normal(rng, extent, jnp.float32)
    if pieces:
        result = result * block_scale(rng, extent, pieces, -0.22, 0.18)
    return jnp.clip(result, -bound, bound).astype(held_as)


def setup_inputs(seed: int = 0) -> dict:
    keys = jax.random.split(jax.random.key(seed), 11)
    incoming = bell_draw(keys[0], (2, RHS, B2, K2), 1.0, 6.0, ((2, 4), (3, 64)), jnp.float32)
    own_field = bell_draw(keys[1], (2, RHS, B1, K1), 1.0, 6.0, ((2, 4), (3, 64)))
    phase_mid = jnp.clip(jax.random.uniform(keys[2], (B1, K1), jnp.float32, -3.140625, 3.140625), -3.140625, 3.140625)
    phase_leaf = jnp.clip(jax.random.uniform(keys[3], (B0, K0), jnp.float32, -3.140625, 3.140625), -3.140625, 3.140625)
    phase_low = jnp.clip(jax.random.uniform(keys[4], (B3, K3), jnp.float32, -3.140625, 3.140625), -3.140625, 3.140625)
    weight_top = jnp.clip(-0.3 + 1.3 * jax.random.uniform(keys[5], (STENCIL, K2), jnp.float32) ** block_scale(keys[5], (STENCIL, K2), ((1, 64),), -0.2, 0.2), -0.3, 1.0)
    weight_leaf = jnp.clip(jax.random.uniform(keys[6], (STENCIL, K1), jnp.float32, -0.3, 1.0), -0.3, 1.0)
    weight_low = jnp.clip(jax.random.uniform(keys[7], (STENCIL, K0), jnp.float32, -0.3, 1.0), -0.3, 1.0)
    offsets = draw_offsets(jax.random.fold_in(keys[10], 71), 0)
    owner = jax.vmap(lambda own: jax.random.permutation(own, N_ANG))(jax.random.split(keys[9], N_BOX)).reshape((N_BOX, N_ANG)).astype(jnp.int32)
    return {"incoming": incoming, "own_field": own_field, "phase_mid": phase_mid, "phase_leaf": phase_leaf, "phase_low": phase_low, "weight_top": weight_top, "weight_leaf": weight_leaf, "weight_low": weight_low, "offsets": offsets, "owner": owner}


def grouped(fine, row):
    shape = fine.shape
    return (fine * row).reshape(shape[:-1] + (shape[-1] // RATIO, RATIO)).sum(axis=-1)


def wrapped(fine, weights, offsets):
    total = jnp.zeros(fine.shape[:-1] + (fine.shape[-1] // RATIO,), jnp.float32)
    for index in range(STENCIL):
        total = total + jnp.roll(grouped(fine, weights[index]), offsets[index], axis=-1)
    return total


def rotate(field, angle):
    cosine = jnp.cos(angle)
    sine = jnp.sin(angle)
    return jnp.stack([field[0] * cosine - field[1] * sine, field[0] * sine + field[1] * cosine])


def reference(incoming, own_field, phase_mid, phase_leaf, phase_low, weight_top, weight_leaf, weight_low, offsets, owner):
    coarse_top = wrapped(incoming, weight_top, offsets)
    children = jnp.repeat(coarse_top, CHILDREN, axis=2)
    mid = rotate(children, phase_mid) + own_field.astype(jnp.float32)
    groups = jnp.arange(N_BOX, dtype=jnp.int32)
    inverse = jnp.zeros((N_BOX, N_ANG), jnp.int32).at[groups[:, None], owner].set(jnp.arange(N_ANG, dtype=jnp.int32)[None, :])
    source = (groups[None, :] * N_ANG + inverse.T).reshape(-1).astype(jnp.int32)
    mid_owned = jnp.take(mid, source, axis=2)
    coarse_leaf = wrapped(mid_owned, weight_leaf, offsets)
    leaves = jnp.repeat(coarse_leaf, CHILDREN, axis=2)
    leaf_field = rotate(leaves, phase_leaf)
    coarse_low = wrapped(leaf_field, weight_low, offsets)
    lows = jnp.repeat(coarse_low, CHILDREN, axis=2)
    return rotate(lows, phase_low)
```

```python
import functools

import jax
import jax.numpy as jnp
from jax import lax
from jax.experimental import pallas as pl
from jax.experimental.pallas import tpu as pltpu
from jax.sharding import PartitionSpec as P

STENCIL = 4
ANG = 64
ROWS = 24
PITCH = 72
NT = (((1,), (1,)), ((), ()))
F32 = jnp.float32
BF16 = jnp.bfloat16
VMEM = pl.BlockSpec(memory_space=pltpu.VMEM)
SMEM = pl.BlockSpec(memory_space=pltpu.SMEM)
ANY = pl.BlockSpec(memory_space=pl.ANY)


def halves(value):
    high = value.astype(BF16)
    return high, (value - high.astype(F32)).astype(BF16)


def iota(shape, dim):
    return lax.broadcasted_iota(jnp.int32, shape, dim)


def product(left, right):
    return lax.dot_general(left, right, NT, preferred_element_type=F32)


def send_kernel(
    incoming, own, phase, weight_top, weight_leaf, offsets, owner, message,
    fine, field, spread_own, coarse, rims, sems,
):
    ang = lax.axis_index("ang")
    box = lax.axis_index("box")
    send_body(ang, box, incoming, own, phase, weight_top, weight_leaf, offsets, owner, message,
              fine, field, spread_own, coarse, rims, sems)


def send_body(
    ang, box, incoming, own, phase, weight_top, weight_leaf, offsets, owner, message,
    fine, field, spread_own, coarse, rims, sems,
):
    get_fine = pltpu.make_async_copy(incoming, fine, sems.at[0])
    get_field = pltpu.make_async_copy(own, field, sems.at[1])
    get_fine.start()
    get_field.start()

    cosine = jnp.cos(phase[...])
    sine = jnp.sin(phase[...])
    lane = iota((64, 128), 1)
    rim_phase = jnp.where(
        (lane < 2) | (lane >= 126),
        cosine,
        jnp.where(lane < 64, pltpu.roll(sine, 2, 1), pltpu.roll(sine, 126, 1)),
    )

    top = []
    for part in range(2):
        at = iota((128, 256), 0)
        group = (iota((128, 256), 1) + 256 * part) // 4
        total = jnp.zeros((128, 256), F32)
        for o in range(STENCIL):
            hit = at == ((group + offsets[o] + 128) & 127)
            total = total + jnp.where(hit, weight_top[o : o + 1, 256 * part : 256 * part + 256], 0.0)
        top.append(jnp.concatenate(halves(total), axis=0))

    row = iota((48, 128), 0)
    inner = row % 24
    first = row < 24
    at = jnp.where(inner < 16, inner + jnp.where(first, 0, 16), inner - 16 + jnp.where(first, 32, -2))
    at = jnp.where(inner < 18, at, -100)
    group = iota((48, 128), 1) // 4
    local = weight_leaf[:, pl.ds(pl.multiple_of(ang * 128, 128), 128)]
    total = jnp.zeros((48, 128), F32)
    for o in range(STENCIL):
        total = total + jnp.where(at == group + offsets[o], local[o : o + 1, :], 0.0)
    high, low = halves(total)
    leaf = jnp.concatenate(
        [jnp.concatenate([high, high], axis=1), jnp.concatenate([low, low], axis=1)], axis=0
    )

    get_fine.wait()
    wide = iota((128, 128), 1)
    for block in range(4):
        rows = fine[block // 2, pl.ds(16 * (block % 2), 16)].reshape(128, 512)
        high, low = halves(rows)
        sums = []
        for part in range(2):
            a = high[:, 256 * part : 256 * part + 256]
            b = low[:, 256 * part : 256 * part + 256]
            y = product(a, top[part]) + product(b, top[part])
            sums.append(y[:, :128] + y[:, 128:])
        coarse[pl.ds(128 * block, 128), :] = jnp.where(
            wide < 2, sums[0], jnp.where(wide >= 126, sums[1], sums[0] + sums[1])
        )
        rims[pl.ds(128 * block, 128), :] = jnp.where(wide >= 64, sums[0], sums[1])

    srow = iota((16, 128), 0)
    slane = iota((16, 128), 1)
    pick = (
        ((srow == 2) & (slane == 0))
        | ((srow == 3) & (slane == 1))
        | ((srow == 10) & (slane == 126))
        | ((srow == 11) & (slane == 127))
    )
    pick = jnp.where(pick, 1.0, 0.0).astype(BF16)
    pick = jnp.concatenate([pick, pick], axis=1)
    rim_tiles = []
    side = iota((8, 128), 1) < 64
    for pair in range(4):
        stacked = []
        for p in (2 * pair, 2 * pair + 1):
            for c in range(2):
                stacked.append(rims[pl.ds(c * 256 + p, 32, stride=8), :])
        high, low = halves(jnp.concatenate(stacked, axis=0))
        got = product(pick, jnp.concatenate([high, low], axis=1))
        right, left = got[:8], got[8:]
        rim_tiles.append(jnp.where(side, right, pltpu.roll(left, 64, 1)))
        rim_tiles.append(jnp.where(side, pltpu.roll(right, 64, 1), left))

    get_field.wait()
    for c in range(2):
        for r in range(32):
            spread_own[pl.ds((c * 32 + r) * PITCH, 64), :] = field[c, r].astype(F32)

    half = iota((24, 128), 1) < 64
    fifth = iota((8, 128), 0) == 4
    for p in range(8):
        x = coarse[pl.ds(p, 32, stride=8), :]
        y = coarse[pl.ds(256 + p, 32, stride=8), :]
        for quad in range(2):
            highs, lows = [], []
            for child in range(4):
                b = 8 * p + 4 * quad + child
                c = cosine[b : b + 1]
                s = sine[b : b + 1]
                ox = spread_own[pl.ds(b, 32, stride=PITCH), :]
                oy = spread_own[pl.ds(32 * PITCH + b, 32, stride=PITCH), :]
                for z in (x * c - y * s + ox, x * s + y * c + oy):
                    high, low = halves(z)
                    highs.append(high)
                    lows.append(low)
            right = jnp.concatenate(
                [jnp.concatenate(highs, axis=0), jnp.concatenate(lows, axis=0)], axis=1
            )
            got = product(leaf, right)
            got = got[:48] + got[48:]
            for pair in range(2):
                a = got[:24, 128 * pair : 128 * pair + 128]
                d = got[24:, 128 * pair : 128 * pair + 128]
                for odd in range(2):
                    b = 8 * p + 4 * quad + 2 * pair + odd
                    if odd:
                        tile = jnp.where(half, pltpu.roll(a, 64, 1), d)
                    else:
                        tile = jnp.where(half, a, pltpu.roll(d, 64, 1))
                    target = owner[box, b]
                    extra = rim_tiles[p] + jnp.where(fifth, rim_phase[b : b + 1], 0.0)
                    message[target, 0:16, :] = tile[:16]
                    message[target, 16:24, :] = tile[16:] + extra


def send(incoming, own, phase, weight_top, weight_leaf, offsets, owner):
    return pl.pallas_call(
        send_kernel,
        out_shape=jax.ShapeDtypeStruct((ANG, ROWS, 128), F32),
        in_specs=[ANY, ANY, VMEM, VMEM, VMEM, SMEM, SMEM],
        out_specs=VMEM,
        scratch_shapes=SEND_SCRATCH,
        compiler_params=pltpu.CompilerParams(vmem_limit_bytes=24 * 2**20),
        name="send",
    )(incoming, own, phase, weight_top, weight_leaf, offsets, owner)


SEND_SCRATCH = [
    pltpu.VMEM((2, 32, 8, 512), F32),
    pltpu.VMEM((2, 32, 64, 128), BF16),
    pltpu.VMEM((64 * PITCH, 128), F32),
    pltpu.VMEM((512, 128), F32),
    pltpu.VMEM((512, 128), F32),
    pltpu.SemaphoreType.DMA((2,)),
]


def compact(source, block, h):
    total = None
    which = iota((8, 128), 1) // 16
    for s in range(8):
        tile = source[:, (2 * block + s // 4) * 128 : (2 * block + s // 4) * 128 + 128]
        shift = (16 * s - (32 * (s % 4) + 16 * h)) % 128
        moved = pltpu.roll(tile, shift, 1) if shift else tile
        total = moved if total is None else jnp.where(which == s, moved, total)
    return total


def table_kernel(
    phase_leaf, phase_low, weight_low, weight_leaf, offsets,
    leaf_cos, leaf_sin, low_cos, low_sin, low_weight, coef, lines,
):
    low_cos[...] = jnp.cos(phase_low[...])
    low_sin[...] = jnp.sin(phase_low[...])
    angles = phase_leaf[...]
    weights = jnp.concatenate([weight_low[...], weight_low[...]], axis=0)
    at = iota((128, 128), 0)
    lane = iota((128, 128), 1)
    for block in range(8):
        columns = []
        for h in range(2):
            angle = compact(angles, block, h)
            leaf_cos[pl.ds(8 * h, 8), pl.ds(128 * block, 128)] = jnp.cos(angle)
            leaf_sin[pl.ds(8 * h, 8), pl.ds(128 * block, 128)] = jnp.sin(angle)
            w = compact(weights, block, h)
            group = 64 * block + (lane // 16) * 8 + 4 * h + (lane % 16) // 4
            total = jnp.zeros((128, 128), F32)
            for o in range(STENCIL):
                total = total + jnp.where(at == ((group + offsets[o] + 512) & 127), w[o : o + 1], 0.0)
            columns.append(jnp.concatenate(halves(total), axis=0))
        low_weight[block] = jnp.concatenate(columns, axis=1)

    for o in range(STENCIL):
        for g in range(ANG):
            lines[pl.ds(64 * o + g, 1), :] = weight_leaf[pl.ds(o, 1), pl.ds(128 * g, 128)]
    side = iota((64, 128), 1) < 64
    for e in range(2):
        each = []
        for o in range(STENCIL):
            part = lines[pl.ds(64 * o, 64), :]
            right = pltpu.roll(jnp.broadcast_to(part[:, e : e + 1], (64, 128)), 63, 0)
            left = pltpu.roll(jnp.broadcast_to(part[:, 126 + e : 127 + e], (64, 128)), 1, 0)
            each.append(jnp.where(side, right, left))
        for m in range(5):
            total = jnp.zeros((64, 128), F32)
            for o in range(STENCIL):
                total = total + jnp.where(offsets[o] == m - 2, each[o], 0.0)
            coef[2 * m + e] = total


def tables(phase_leaf, phase_low, weight_low, weight_leaf, offsets):
    return pl.pallas_call(
        table_kernel,
        out_shape=[
            jax.ShapeDtypeStruct((16, 1024), F32),
            jax.ShapeDtypeStruct((16, 1024), F32),
            jax.ShapeDtypeStruct((64, 512), F32),
            jax.ShapeDtypeStruct((64, 512), F32),
            jax.ShapeDtypeStruct((8, 256, 256), BF16),
            jax.ShapeDtypeStruct((10, 64, 128), F32),
        ],
        in_specs=[VMEM, VMEM, VMEM, VMEM, SMEM],
        out_specs=[VMEM] * 6,
        scratch_shapes=[pltpu.VMEM((256, 128), F32)],
        compiler_params=pltpu.CompilerParams(vmem_limit_bytes=16 * 2**20),
        name="tables",
    )(phase_leaf, phase_low, weight_low, weight_leaf, offsets)


def receive_kernel(
    got, leaf_cos, leaf_sin, low_cos, low_sin, low_weight, coef, out,
    lines, added, parts, low, result, sems,
):
    side = iota((64, 128), 1) < 64
    lane = iota((64, 128), 1)

    def line(i):
        return lines[pl.ds(i, 64, stride=8), :]

    for s in range(ANG):
        lines[pl.ds(8 * s, 8), :] = got[s, 16:24, :]
    cs = line(4)

    def spread(right, left):
        right = pltpu.roll(jnp.broadcast_to(cs[:, right : right + 1], (64, 128)), 63, 0)
        left = pltpu.roll(jnp.broadcast_to(cs[:, left : left + 1], (64, 128)), 1, 0)
        return jnp.where(side, right, left)

    turned = []
    for e in range(2):
        t = line(2 + e)
        c = spread(e, 126 + e)
        s = spread(2 + e, 124 + e)
        is_x = (lane & 63) < 32
        other = jnp.where(is_x, pltpu.roll(t, 96, 1), pltpu.roll(t, 32, 1))
        turned.append(t * c + other * jnp.where(is_x, -s, s))
    e = [coef[2 * m] * turned[0] + coef[2 * m + 1] * turned[1] for m in range(5)]
    l0, l1 = line(0), line(1)
    e[1] = e[1] + jnp.where(side, 0.0, l0)
    e[2] = e[2] + jnp.where(side, l0, l1)
    e[3] = e[3] + jnp.where(side, l1, 0.0)

    def before(v):
        return pltpu.roll(v, 1, 0)

    def after(v):
        return pltpu.roll(v, 63, 0)

    def swap(v):
        return pltpu.roll(v, 64, 1)

    added[...] = jnp.zeros_like(added)
    rows = {
        0: jnp.where(side, before(e[2]) + swap(e[3]), 0.0),
        1: jnp.where(side, before(e[3]) + swap(e[4]), 0.0),
        2: jnp.where(side, before(e[4]), 0.0),
        13: jnp.where(side, 0.0, after(e[0])),
        14: jnp.where(side, 0.0, after(e[1]) + swap(e[0])),
        15: jnp.where(side, 0.0, after(e[2]) + swap(e[1])),
    }
    for i, value in rows.items():
        added[pl.ds(i, 64, stride=16), :] = value

    for block in range(8):
        tile = got[pl.ds(8 * block, 8), 0:16, :].reshape(128, 128) + added[pl.ds(128 * block, 128), :]
        flat = tile.T
        highs, lows = [], []
        for child in range(8):
            pair = []
            for h in range(2):
                x = flat[64 * h : 64 * h + 32]
                y = flat[64 * h + 32 : 64 * h + 64]
                c = leaf_cos[pl.ds(8 * h + child, 1), pl.ds(128 * block, 128)]
                s = leaf_sin[pl.ds(8 * h + child, 1), pl.ds(128 * block, 128)]
                pair.append((halves(x * c - y * s), halves(x * s + y * c)))
            for component in range(2):
                highs.append(jnp.concatenate([pair[0][component][0], pair[1][component][0]], axis=1))
                lows.append(jnp.concatenate([pair[0][component][1], pair[1][component][1]], axis=1))
        w = low_weight[block]
        y = product(jnp.concatenate(highs, axis=0), w) + product(jnp.concatenate(lows, axis=0), w)
        parts[block] = y[:, :128] + y[:, 128:]

    wide = iota((512, 128), 1)
    for t in range(4):
        here, there = parts[2 * t], parts[2 * t + 1]
        total = jnp.where(
            wide < 2,
            here + parts[(2 * t + 7) % 8],
            jnp.where(wide >= 126, there + parts[(2 * t + 2) % 8], here + there),
        )
        low[:, pl.ds(128 * t, 128)] = total

    def copies(r):
        return [pltpu.make_async_copy(result.at[c, r], out.at[c, r], sems.at[c, r]) for c in range(2)]

    def step(r, carry):
        for child in range(8):
            x = low[pl.ds(64 * child + r, 1), :]
            y = low[pl.ds(64 * child + 32 + r, 1), :]
            c = low_cos[pl.ds(8 * child, 8), :]
            s = low_sin[pl.ds(8 * child, 8), :]
            result[0, r, pl.ds(8 * child, 8), :] = x * c - y * s
            result[1, r, pl.ds(8 * child, 8), :] = x * s + y * c
        for copy in copies(r):
            copy.start()
        return carry

    lax.fori_loop(0, 32, step, 0)

    def finish(r, carry):
        for copy in copies(r):
            copy.wait()
        return carry

    lax.fori_loop(0, 32, finish, 0)


RECEIVE_SCRATCH = [
    pltpu.VMEM((512, 128), F32),
    pltpu.VMEM((1024, 128), F32),
    pltpu.VMEM((8, 512, 128), F32),
    pltpu.VMEM((512, 512), F32),
    pltpu.VMEM((2, 32, 64, 512), F32),
    pltpu.SemaphoreType.DMA((2, 32)),
]


def receive(got, ready):
    return pl.pallas_call(
        receive_kernel,
        out_shape=jax.ShapeDtypeStruct((2, 32, 64, 512), F32),
        in_specs=[VMEM] * 7,
        out_specs=ANY,
        scratch_shapes=RECEIVE_SCRATCH,
        compiler_params=pltpu.CompilerParams(vmem_limit_bytes=32 * 2**20),
        name="receive",
    )(got, *ready)


def body(
    incoming, own_field, phase_mid, phase_leaf, phase_low,
    weight_top, weight_leaf, weight_low, offsets, owner,
):
    message = send(incoming, own_field, phase_mid, weight_top, weight_leaf, offsets, owner)
    got = lax.all_to_all(message, "ang", split_axis=0, concat_axis=0, tiled=True)
    ready = tables(phase_leaf, phase_low, weight_low, weight_leaf, offsets)
    return receive(got, ready)


def solution(mesh):
    placed = (
        P(None, None, "box", "ang"),
        P(None, None, "box", "ang"),
        P("box", "ang"),
        P(("ang", "box"), None),
        P(("ang", "box"), None),
        P(None, "ang"),
        P(),
        P(),
        P(),
        P(),
    )
    return jax.shard_map(
        body,
        mesh=mesh,
        in_specs=placed,
        out_specs=P(None, None, ("ang", "box"), None),
        check_vma=False,
    )
```

```python
import functools

import jax
import jax.numpy as jnp
from jax import lax
from jax.experimental import pallas as pl
from jax.experimental.pallas import tpu as pltpu
from jax.sharding import PartitionSpec as P

STENCIL = 4
ANG = 64
ROWS = 21
PITCH = 72
NT = (((1,), (1,)), ((), ()))
F32 = jnp.float32
BF16 = jnp.bfloat16
VMEM = pl.BlockSpec(memory_space=pltpu.VMEM)
SMEM = pl.BlockSpec(memory_space=pltpu.SMEM)
HBM = pl.BlockSpec(memory_space=pltpu.HBM)


def halves(value):
    high = value.astype(BF16)
    return high, (value - high.astype(F32)).astype(BF16)


def iota(shape, dim):
    return lax.broadcasted_iota(jnp.int32, shape, dim)


def product(left, right):
    return lax.dot_general(left, right, NT, preferred_element_type=F32)


def send_kernel(
    incoming, own, all_phase, all_top, all_leaf, all_offsets, all_owner, message,
    fine, field, phase, weight_top, local, offsets, owner, spread_own, coarse, rims, sems,
):
    ang = lax.axis_index("ang")
    box = lax.axis_index("box")
    small = [
        pltpu.make_async_copy(source, target, sems.at[i])
        for i, (source, target) in enumerate(
            (
                (all_phase, phase),
                (all_offsets, offsets),
                (all_top, weight_top),
                (all_leaf.at[:, pl.ds(pl.multiple_of(ang * 128, 128), 128)], local),
                (all_owner, owner),
            )
        )
    ]
    get_fine = [
        pltpu.make_async_copy(incoming.at[i // 2, pl.ds(16 * (i % 2), 16)], fine.at[i], sems.at[5 + i])
        for i in range(4)
    ]
    get_field = [pltpu.make_async_copy(own.at[c], field.at[c], sems.at[9 + c]) for c in range(2)]
    for copy in small + get_fine + get_field:
        copy.start()

    small[0].wait()
    cosine = jnp.cos(phase[...])
    sine = jnp.sin(phase[...])
    lane = iota((64, 128), 1)
    rim_phase = jnp.where(
        (lane < 2) | (lane >= 126),
        cosine,
        jnp.where(lane < 64, pltpu.roll(sine, 2, 1), pltpu.roll(sine, 126, 1)),
    )

    small[1].wait()
    small[2].wait()
    top = []
    for part in range(2):
        at = iota((128, 256), 0)
        group = (iota((128, 256), 1) + 256 * part) // 4
        total = jnp.zeros((128, 256), F32)
        for o in range(STENCIL):
            hit = at == ((group + offsets[o] + 128) & 127)
            total = total + jnp.where(hit, weight_top[o : o + 1, 256 * part : 256 * part + 256], 0.0)
        top.append(jnp.concatenate(halves(total), axis=0))

    row = iota((48, 128), 0)
    inner = row % 24
    first = row < 24
    at = jnp.where(inner < 16, inner + jnp.where(first, 0, 16), inner - 16 + jnp.where(first, 32, -2))
    at = jnp.where(inner < 18, at, -100)
    group = iota((48, 128), 1) // 4
    small[3].wait()
    total = jnp.zeros((48, 128), F32)
    for o in range(STENCIL):
        total = total + jnp.where(at == group + offsets[o], local[o : o + 1, :], 0.0)
    high, low = halves(total)
    leaf = jnp.concatenate(
        [jnp.concatenate([high, high], axis=1), jnp.concatenate([low, low], axis=1)], axis=0
    )

    wide = iota((128, 128), 1)
    for block in range(4):
        get_fine[block].wait()
        rows = fine[block].reshape(128, 512)
        high, low = halves(rows)
        sums = []
        for part in range(2):
            a = high[:, 256 * part : 256 * part + 256]
            b = low[:, 256 * part : 256 * part + 256]
            y = product(a, top[part]) + product(b, top[part])
            sums.append(y[:, :128] + y[:, 128:])
        coarse[pl.ds(128 * block, 128), :] = jnp.where(
            wide < 2, sums[0], jnp.where(wide >= 126, sums[1], sums[0] + sums[1])
        )
        rims[pl.ds(128 * block, 128), :] = jnp.where(wide >= 64, sums[0], sums[1])

    srow = iota((16, 128), 0)
    slane = iota((16, 128), 1)
    pick = (
        ((srow == 2) & (slane == 0))
        | ((srow == 3) & (slane == 1))
        | ((srow == 10) & (slane == 126))
        | ((srow == 11) & (slane == 127))
    )
    pick = jnp.where(pick, 1.0, 0.0).astype(BF16)
    pick = jnp.concatenate([pick, pick], axis=1)
    rim_tiles = []
    side = iota((8, 128), 1) < 64
    for pair in range(4):
        stacked = []
        for p in (2 * pair, 2 * pair + 1):
            for c in range(2):
                stacked.append(rims[pl.ds(c * 256 + p, 32, stride=8), :])
        high, low = halves(jnp.concatenate(stacked, axis=0))
        got = product(pick, jnp.concatenate([high, low], axis=1))
        right, left = got[:8], got[8:]
        rim_tiles.append(jnp.where(side, right, pltpu.roll(left, 64, 1)))
        rim_tiles.append(jnp.where(side, pltpu.roll(right, 64, 1), left))

    for c in range(2):
        get_field[c].wait()
        for r in range(32):
            spread_own[pl.ds((c * 32 + r) * PITCH, 64), :] = field[c, r].astype(F32)

    small[4].wait()
    half = iota((24, 128), 1) < 64
    fifth = iota((8, 128), 0) == 4
    for p in range(8):
        x = coarse[pl.ds(p, 32, stride=8), :]
        y = coarse[pl.ds(256 + p, 32, stride=8), :]
        for quad in range(2):
            highs, lows = [], []
            for child in range(4):
                b = 8 * p + 4 * quad + child
                c = cosine[b : b + 1]
                s = sine[b : b + 1]
                ox = spread_own[pl.ds(b, 32, stride=PITCH), :]
                oy = spread_own[pl.ds(32 * PITCH + b, 32, stride=PITCH), :]
                for z in (x * c - y * s + ox, x * s + y * c + oy):
                    high, low = halves(z)
                    highs.append(high)
                    lows.append(low)
            right = jnp.concatenate(
                [jnp.concatenate(highs, axis=0), jnp.concatenate(lows, axis=0)], axis=1
            )
            got = product(leaf, right)
            got = got[:48] + got[48:]
            for pair in range(2):
                a = got[:24, 128 * pair : 128 * pair + 128]
                d = got[24:, 128 * pair : 128 * pair + 128]
                for odd in range(2):
                    b = 8 * p + 4 * quad + 2 * pair + odd
                    if odd:
                        tile = jnp.where(half, pltpu.roll(a, 64, 1), d)
                    else:
                        tile = jnp.where(half, a, pltpu.roll(d, 64, 1))
                    target = owner[box, b] * ROWS
                    extra = rim_tiles[p] + jnp.where(fifth, rim_phase[b : b + 1], 0.0)
                    message[pl.ds(target, 16), :] = tile[:16]
                    message[pl.ds(target + 16, 5), :] = (tile[16:] + extra)[:5]


def send(incoming, own, phase, weight_top, weight_leaf, offsets, owner):
    return pl.pallas_call(
        send_kernel,
        out_shape=jax.ShapeDtypeStruct((ANG * ROWS, 128), F32),
        in_specs=[HBM] * 7,
        out_specs=VMEM,
        scratch_shapes=SEND_SCRATCH,
        compiler_params=pltpu.CompilerParams(vmem_limit_bytes=24 * 2**20),
        name="send",
    )(incoming, own, phase, weight_top, weight_leaf, offsets, owner)


SEND_SCRATCH = [
    pltpu.VMEM((4, 16, 8, 512), F32),
    pltpu.VMEM((2, 32, 64, 128), BF16),
    pltpu.VMEM((64, 128), F32),
    pltpu.VMEM((4, 512), F32),
    pltpu.VMEM((4, 128), F32),
    pltpu.SMEM((4,), jnp.int32),
    pltpu.SMEM((4, 64), jnp.int32),
    pltpu.VMEM((64 * PITCH, 128), F32),
    pltpu.VMEM((512, 128), F32),
    pltpu.VMEM((512, 128), F32),
    pltpu.SemaphoreType.DMA((11,)),
]


def compact(source, block, h):
    total = None
    which = iota((8, 128), 1) // 16
    for s in range(8):
        tile = source[:, (2 * block + s // 4) * 128 : (2 * block + s // 4) * 128 + 128]
        shift = (16 * s - (32 * (s % 4) + 16 * h)) % 128
        moved = pltpu.roll(tile, shift, 1) if shift else tile
        total = moved if total is None else jnp.where(which == s, moved, total)
    return total


def table_kernel(
    phase_leaf, phase_low, weight_low, weight_leaf, offsets,
    leaf_cos, leaf_sin, low_cos, low_sin, low_weight, coef, lines,
):
    low_cos[...] = jnp.cos(phase_low[...])
    low_sin[...] = jnp.sin(phase_low[...])
    angles = phase_leaf[...]
    weights = jnp.concatenate([weight_low[...], weight_low[...]], axis=0)
    at = iota((128, 128), 0)
    lane = iota((128, 128), 1)
    for block in range(8):
        columns = []
        for h in range(2):
            angle = compact(angles, block, h)
            leaf_cos[pl.ds(8 * h, 8), pl.ds(128 * block, 128)] = jnp.cos(angle)
            leaf_sin[pl.ds(8 * h, 8), pl.ds(128 * block, 128)] = jnp.sin(angle)
            w = compact(weights, block, h)
            group = 64 * block + (lane // 16) * 8 + 4 * h + (lane % 16) // 4
            total = jnp.zeros((128, 128), F32)
            for o in range(STENCIL):
                total = total + jnp.where(at == ((group + offsets[o] + 512) & 127), w[o : o + 1], 0.0)
            columns.append(jnp.concatenate(halves(total), axis=0))
        low_weight[block] = jnp.concatenate(columns, axis=1)

    for o in range(STENCIL):
        for g in range(ANG):
            lines[pl.ds(64 * o + g, 1), :] = weight_leaf[pl.ds(o, 1), pl.ds(128 * g, 128)]
    side = iota((64, 128), 1) < 64
    for e in range(2):
        each = []
        for o in range(STENCIL):
            part = lines[pl.ds(64 * o, 64), :]
            right = pltpu.roll(jnp.broadcast_to(part[:, e : e + 1], (64, 128)), 63, 0)
            left = pltpu.roll(jnp.broadcast_to(part[:, 126 + e : 127 + e], (64, 128)), 1, 0)
            each.append(jnp.where(side, right, left))
        for m in range(5):
            total = jnp.zeros((64, 128), F32)
            for o in range(STENCIL):
                total = total + jnp.where(offsets[o] == m - 2, each[o], 0.0)
            coef[2 * m + e] = total


def tables(phase_leaf, phase_low, weight_low, weight_leaf, offsets):
    return pl.pallas_call(
        table_kernel,
        out_shape=[
            jax.ShapeDtypeStruct((16, 1024), F32),
            jax.ShapeDtypeStruct((16, 1024), F32),
            jax.ShapeDtypeStruct((64, 512), F32),
            jax.ShapeDtypeStruct((64, 512), F32),
            jax.ShapeDtypeStruct((8, 256, 256), BF16),
            jax.ShapeDtypeStruct((10, 64, 128), F32),
        ],
        in_specs=[VMEM, VMEM, VMEM, VMEM, SMEM],
        out_specs=[VMEM] * 6,
        scratch_shapes=[pltpu.VMEM((256, 128), F32)],
        compiler_params=pltpu.CompilerParams(vmem_limit_bytes=16 * 2**20),
        name="tables",
    )(phase_leaf, phase_low, weight_low, weight_leaf, offsets)


def receive_kernel(
    got, leaf_cos, leaf_sin, low_cos, low_sin, low_weight, coef, out,
    lines, added, parts, low, result, sems,
):
    side = iota((64, 128), 1) < 64
    lane = iota((64, 128), 1)

    def line(i):
        return lines[pl.ds(i, 64, stride=8), :]

    for s in range(ANG):
        lines[pl.ds(8 * s, 5), :] = got[pl.ds(ROWS * s + 16, 5), :]
    cs = line(4)

    def spread(right, left):
        right = pltpu.roll(jnp.broadcast_to(cs[:, right : right + 1], (64, 128)), 63, 0)
        left = pltpu.roll(jnp.broadcast_to(cs[:, left : left + 1], (64, 128)), 1, 0)
        return jnp.where(side, right, left)

    turned = []
    for e in range(2):
        t = line(2 + e)
        c = spread(e, 126 + e)
        s = spread(2 + e, 124 + e)
        is_x = (lane & 63) < 32
        other = jnp.where(is_x, pltpu.roll(t, 96, 1), pltpu.roll(t, 32, 1))
        turned.append(t * c + other * jnp.where(is_x, -s, s))
    e = [coef[2 * m] * turned[0] + coef[2 * m + 1] * turned[1] for m in range(5)]
    l0, l1 = line(0), line(1)
    e[1] = e[1] + jnp.where(side, 0.0, l0)
    e[2] = e[2] + jnp.where(side, l0, l1)
    e[3] = e[3] + jnp.where(side, l1, 0.0)

    def before(v):
        return pltpu.roll(v, 1, 0)

    def after(v):
        return pltpu.roll(v, 63, 0)

    def swap(v):
        return pltpu.roll(v, 64, 1)

    added[...] = jnp.zeros_like(added)
    rows = {
        0: jnp.where(side, before(e[2]) + swap(e[3]), 0.0),
        1: jnp.where(side, before(e[3]) + swap(e[4]), 0.0),
        2: jnp.where(side, before(e[4]), 0.0),
        13: jnp.where(side, 0.0, after(e[0])),
        14: jnp.where(side, 0.0, after(e[1]) + swap(e[0])),
        15: jnp.where(side, 0.0, after(e[2]) + swap(e[1])),
    }
    for i, value in rows.items():
        added[pl.ds(i, 64, stride=16), :] = value

    for block in range(8):
        tile = jnp.concatenate([got[pl.ds(ROWS * (8 * block + s), 16), :] for s in range(8)], axis=0)
        tile = tile + added[pl.ds(128 * block, 128), :]
        flat = tile.T
        highs, lows = [], []
        for child in range(8):
            pair = []
            for h in range(2):
                x = flat[64 * h : 64 * h + 32]
                y = flat[64 * h + 32 : 64 * h + 64]
                c = leaf_cos[pl.ds(8 * h + child, 1), pl.ds(128 * block, 128)]
                s = leaf_sin[pl.ds(8 * h + child, 1), pl.ds(128 * block, 128)]
                pair.append((halves(x * c - y * s), halves(x * s + y * c)))
            for component in range(2):
                highs.append(jnp.concatenate([pair[0][component][0], pair[1][component][0]], axis=1))
                lows.append(jnp.concatenate([pair[0][component][1], pair[1][component][1]], axis=1))
        w = low_weight[block]
        y = product(jnp.concatenate(highs, axis=0), w) + product(jnp.concatenate(lows, axis=0), w)
        parts[block] = y[:, :128] + y[:, 128:]

    wide = iota((512, 128), 1)
    for t in range(4):
        here, there = parts[2 * t], parts[2 * t + 1]
        total = jnp.where(
            wide < 2,
            here + parts[(2 * t + 7) % 8],
            jnp.where(wide >= 126, there + parts[(2 * t + 2) % 8], here + there),
        )
        low[:, pl.ds(128 * t, 128)] = total

    def copies(r):
        return [pltpu.make_async_copy(result.at[c, r], out.at[c, r], sems.at[c, r]) for c in range(2)]

    def step(r, carry):
        for child in range(8):
            x = low[pl.ds(64 * child + r, 1), :]
            y = low[pl.ds(64 * child + 32 + r, 1), :]
            c = low_cos[pl.ds(8 * child, 8), :]
            s = low_sin[pl.ds(8 * child, 8), :]
            result[0, r, pl.ds(8 * child, 8), :] = x * c - y * s
            result[1, r, pl.ds(8 * child, 8), :] = x * s + y * c
        for copy in copies(r):
            copy.start()
        return carry

    lax.fori_loop(0, 32, step, 0)

    def finish(r, carry):
        for copy in copies(r):
            copy.wait()
        return carry

    lax.fori_loop(0, 32, finish, 0)


RECEIVE_SCRATCH = [
    pltpu.VMEM((512, 128), F32),
    pltpu.VMEM((1024, 128), F32),
    pltpu.VMEM((8, 512, 128), F32),
    pltpu.VMEM((512, 512), F32),
    pltpu.VMEM((2, 32, 64, 512), F32),
    pltpu.SemaphoreType.DMA((2, 32)),
]


def receive(got, ready):
    return pl.pallas_call(
        receive_kernel,
        out_shape=jax.ShapeDtypeStruct((2, 32, 64, 512), F32),
        in_specs=[VMEM] * 7,
        out_specs=HBM,
        scratch_shapes=RECEIVE_SCRATCH,
        compiler_params=pltpu.CompilerParams(vmem_limit_bytes=32 * 2**20),
        name="receive",
    )(got, *ready)


def body(
    incoming, own_field, phase_mid, phase_leaf, phase_low,
    weight_top, weight_leaf, weight_low, offsets, owner,
):
    incoming, own_field, phase_mid, phase_leaf, phase_low, weight_top, weight_leaf, weight_low, offsets, owner = (
        pltpu.with_memory_space_constraint(value, pltpu.HBM)
        for value in (
            incoming, own_field, phase_mid, phase_leaf, phase_low,
            weight_top, weight_leaf, weight_low, offsets, owner,
        )
    )
    message = send(incoming, own_field, phase_mid, weight_top, weight_leaf, offsets, owner)
    message = message.reshape(ANG, 1, ROWS * 128)
    got = lax.all_to_all(message, "ang", split_axis=0, concat_axis=0, tiled=True)
    got = got.reshape(ANG * ROWS, 128)
    ready = tables(phase_leaf, phase_low, weight_low, weight_leaf, offsets)
    return receive(got, ready)


def solution(mesh):
    placed = (
        P(None, None, "box", "ang"),
        P(None, None, "box", "ang"),
        P("box", "ang"),
        P(("ang", "box"), None),
        P(("ang", "box"), None),
        P(None, "ang"),
        P(),
        P(),
        P(),
        P(),
    )
    return jax.shard_map(
        body,
        mesh=mesh,
        in_specs=placed,
        out_specs=P(None, None, ("ang", "box"), None),
        check_vma=False,
    )
```

```python
import functools

import jax
import jax.numpy as jnp
from jax import lax
from jax.experimental import pallas as pl
from jax.experimental.pallas import tpu as pltpu
from jax.sharding import PartitionSpec as P

STENCIL = 4
ANG = 64
ROWS = 21
PITCH = 72
COUNT = 16
PER = 16
CHUNK = 16
NT = (((1,), (1,)), ((), ()))
F32 = jnp.float32
BF16 = jnp.bfloat16
VMEM = pl.BlockSpec(memory_space=pltpu.VMEM)
SMEM = pl.BlockSpec(memory_space=pltpu.SMEM)
HBM = pl.BlockSpec(memory_space=pltpu.HBM)


def halves(value):
    high = value.astype(BF16)
    return high, (value - high.astype(F32)).astype(BF16)


def iota(shape, dim):
    return lax.broadcasted_iota(jnp.int32, shape, dim)


def turn(angle):
    count = jnp.floor(angle * 0.6366197723675814 + 0.5)
    rest = angle - count * 1.5703125
    rest = rest - count * 4.837512969970703e-4
    rest = rest - count * 7.549789954891e-8
    square = rest * rest
    sine = ((-1.9515295891e-4 * square + 8.3321608736e-3) * square - 1.6666654611e-1) * square * rest + rest
    cosine = ((2.443315711809948e-5 * square - 1.388731625493765e-3) * square + 4.166664568298827e-2) * square
    cosine = cosine * square - 0.5 * square + 1.0
    quarter = count.astype(jnp.int32)
    odd = (quarter & 1) == 1
    first = jnp.where(odd, sine, cosine)
    second = jnp.where(odd, cosine, sine)
    return (
        jnp.where(((quarter + 1) & 2) == 2, -first, first),
        jnp.where((quarter & 2) == 2, -second, second),
    )


def window(hits, weights):
    total = None
    for o in range(STENCIL):
        term = jnp.where(hits[o], weights[o], 0.0)
        total = term if total is None else total + term
    return halves(total)


def placed(piece, start):
    begin = (start - 8) % 128
    zero = jnp.zeros((80, 128), BF16)
    if begin + 48 <= 128:
        return jnp.concatenate([zero[:begin], piece, zero[begin:]], axis=0)
    over = begin + 48 - 128
    return jnp.concatenate([piece[48 - over :], zero, piece[: 48 - over]], axis=0)


def product(left, right):
    return lax.dot_general(left, right, NT, preferred_element_type=F32)


def send_kernel(
    incoming, own, all_phase, all_top, all_leaf, all_offsets, all_owner, message,
    fine, field, phase, weight_top, local, offsets, owner, spread_own, coarse, rims, sems,
):
    ang = lax.axis_index("ang")
    box = lax.axis_index("box")
    small = [
        pltpu.make_async_copy(source, target, sems.at[i])
        for i, (source, target) in enumerate(
            (
                (all_phase, phase),
                (all_offsets, offsets),
                (all_top, weight_top),
                (all_leaf.at[:, pl.ds(pl.multiple_of(ang * 128, 128), 128)], local),
                (all_owner, owner),
            )
        )
    ]
    get_fine = [
        pltpu.make_async_copy(incoming.at[i // 2, pl.ds(16 * (i % 2), 16)], fine.at[i], sems.at[5 + i])
        for i in range(4)
    ]
    get_field = [pltpu.make_async_copy(own.at[c], field.at[c], sems.at[9 + c]) for c in range(2)]
    for copy in small + get_fine + get_field:
        copy.start()

    small[0].wait()
    cosine, sine = turn(phase[...])
    lane = iota((64, 128), 1)
    rim_phase = jnp.where(
        (lane < 2) | (lane >= 126),
        cosine,
        jnp.where(lane < 64, pltpu.roll(sine, 2, 1), pltpu.roll(sine, 126, 1)),
    )

    small[1].wait()
    small[2].wait()
    apart = iota((48, 128), 0) - 8 - iota((48, 128), 1) // 4
    hits = [apart == offsets[o] for o in range(STENCIL)]
    top = []
    for part in range(2):
        highs, lows = [], []
        for k in (2 * part, 2 * part + 1):
            high, low = window(hits, [weight_top[o : o + 1, 128 * k : 128 * k + 128] for o in range(STENCIL)])
            highs.append(placed(high, 32 * k))
            lows.append(placed(low, 32 * k))
        top.append(jnp.concatenate([jnp.concatenate(highs, axis=1), jnp.concatenate(lows, axis=1)], axis=0))

    row = iota((48, 128), 0)
    inner = row % 24
    first = row < 24
    at = jnp.where(inner < 16, inner + jnp.where(first, 0, 16), inner - 16 + jnp.where(first, 32, -2))
    at = jnp.where(inner < 18, at, -100)
    apart = at - iota((48, 128), 1) // 4
    small[3].wait()
    high, low = window(
        [apart == offsets[o] for o in range(STENCIL)], [local[o : o + 1, :] for o in range(STENCIL)]
    )
    leaf = jnp.concatenate(
        [jnp.concatenate([high, high], axis=1), jnp.concatenate([low, low], axis=1)], axis=0
    )

    wide = iota((128, 128), 1)
    for block in range(4):
        get_fine[block].wait()
        rows = fine[block].reshape(128, 512)
        high, low = halves(rows)
        sums = []
        for part in range(2):
            a = high[:, 256 * part : 256 * part + 256]
            b = low[:, 256 * part : 256 * part + 256]
            y = product(a, top[part]) + product(b, top[part])
            sums.append(y[:, :128] + y[:, 128:])
        coarse[pl.ds(128 * block, 128), :] = jnp.where(
            wide < 2, sums[0], jnp.where(wide >= 126, sums[1], sums[0] + sums[1])
        )
        rims[pl.ds(128 * block, 128), :] = jnp.where(wide >= 64, sums[0], sums[1])

    srow = iota((16, 128), 0)
    slane = iota((16, 128), 1)
    pick = (
        ((srow == 2) & (slane == 0))
        | ((srow == 3) & (slane == 1))
        | ((srow == 10) & (slane == 126))
        | ((srow == 11) & (slane == 127))
    )
    pick = jnp.where(pick, 1.0, 0.0).astype(BF16)
    pick = jnp.concatenate([pick, pick], axis=1)
    rim_tiles = []
    side = iota((8, 128), 1) < 64
    for pair in range(4):
        stacked = []
        for p in (2 * pair, 2 * pair + 1):
            for c in range(2):
                stacked.append(rims[pl.ds(c * 256 + p, 32, stride=8), :])
        high, low = halves(jnp.concatenate(stacked, axis=0))
        got = product(pick, jnp.concatenate([high, low], axis=1))
        right, left = got[:8], got[8:]
        rim_tiles.append(jnp.where(side, right, pltpu.roll(left, 64, 1)))
        rim_tiles.append(jnp.where(side, pltpu.roll(right, 64, 1), left))

    for c in range(2):
        get_field[c].wait()
        for r in range(32):
            spread_own[pl.ds((c * 32 + r) * PITCH, 64), :] = field[c, r].astype(F32)

    small[4].wait()
    half = iota((24, 128), 1) < 64
    fifth = iota((8, 128), 0) == 4
    for p in range(8):
        x = coarse[pl.ds(p, 32, stride=8), :]
        y = coarse[pl.ds(256 + p, 32, stride=8), :]
        for quad in range(2):
            highs, lows = [], []
            for child in range(4):
                b = 8 * p + 4 * quad + child
                c = cosine[b : b + 1]
                s = sine[b : b + 1]
                ox = spread_own[pl.ds(b, 32, stride=PITCH), :]
                oy = spread_own[pl.ds(32 * PITCH + b, 32, stride=PITCH), :]
                for z in (x * c - y * s + ox, x * s + y * c + oy):
                    high, low = halves(z)
                    highs.append(high)
                    lows.append(low)
            right = jnp.concatenate(
                [jnp.concatenate(highs, axis=0), jnp.concatenate(lows, axis=0)], axis=1
            )
            got = product(leaf, right)
            got = got[:48] + got[48:]
            for pair in range(2):
                a = got[:24, 128 * pair : 128 * pair + 128]
                d = got[24:, 128 * pair : 128 * pair + 128]
                for odd in range(2):
                    b = 8 * p + 4 * quad + 2 * pair + odd
                    if odd:
                        tile = jnp.where(half, pltpu.roll(a, 64, 1), d)
                    else:
                        tile = jnp.where(half, a, pltpu.roll(d, 64, 1))
                    target = owner[box, b] * ROWS
                    extra = rim_tiles[p] + jnp.where(fifth, rim_phase[b : b + 1], 0.0)
                    message[pl.ds(target, 16), :] = tile[:16]
                    message[pl.ds(target + 16, 5), :] = (tile[16:] + extra)[:5]


def send(incoming, own, phase, weight_top, weight_leaf, offsets, owner):
    return pl.pallas_call(
        send_kernel,
        out_shape=jax.ShapeDtypeStruct((ANG * ROWS, 128), F32),
        in_specs=[HBM] * 7,
        out_specs=VMEM,
        scratch_shapes=SEND_SCRATCH,
        compiler_params=pltpu.CompilerParams(vmem_limit_bytes=24 * 2**20),
        name="send",
    )(incoming, own, phase, weight_top, weight_leaf, offsets, owner)


SEND_SCRATCH = [
    pltpu.VMEM((4, 16, 8, 512), F32),
    pltpu.VMEM((2, 32, 64, 128), BF16),
    pltpu.VMEM((64, 128), F32),
    pltpu.VMEM((4, 512), F32),
    pltpu.VMEM((4, 128), F32),
    pltpu.SMEM((4,), jnp.int32),
    pltpu.SMEM((4, 64), jnp.int32),
    pltpu.VMEM((64 * PITCH, 128), F32),
    pltpu.VMEM((512, 128), F32),
    pltpu.VMEM((512, 128), F32),
    pltpu.SemaphoreType.DMA((11,)),
]


def table_kernel(
    phase_leaf, phase_low, weight_low, weight_leaf, offsets,
    leaf_cos, leaf_sin, low_cos, low_sin, low_weight, coef, lines,
):
    low_cos[...], low_sin[...] = turn(phase_low[...])
    row, column = iota((256, 256), 0), iota((256, 256), 1)
    order = jnp.where(column == (row % 8) * 32 + (row // 128) * 16 + (row % 128) // 8, 1.0, 0.0).astype(BF16)
    stacked = []
    for block in range(8):
        stacked.append(phase_leaf[:, 256 * block : 256 * block + 256])
        stacked.append(weight_low[:, 256 * block : 256 * block + 256])
        stacked.append(weight_low[:, 256 * block : 256 * block + 256])
    stacked = jnp.concatenate(stacked, axis=0)
    high, rest = stacked.astype(BF16), stacked
    rest = rest - high.astype(F32)
    middle = rest.astype(BF16)
    low = (rest - middle.astype(F32)).astype(BF16)
    sorted_ = product(high, order) + product(middle, order) + product(low, order)
    at, lane = iota((128, 128), 0), iota((128, 128), 1)
    for block in range(8):
        columns = []
        for h in range(2):
            part = sorted_[16 * block : 16 * block + 16, 128 * h : 128 * h + 128]
            to = pl.ds(128 * block, 128)
            leaf_cos[pl.ds(8 * h, 8), to], leaf_sin[pl.ds(8 * h, 8), to] = turn(part[:8])
            apart = (at - (64 * block + (lane % 8) * 8 + 4 * h + lane // 32)) & 127
            hits = [apart == (offsets[o] & 127) for o in range(STENCIL)]
            columns.append(jnp.concatenate(window(hits, [part[8 + o : 9 + o] for o in range(STENCIL)]), axis=0))
        low_weight[block] = jnp.concatenate(columns, axis=1)

    for o in range(STENCIL):
        for g in range(ANG):
            lines[pl.ds(64 * o + g, 1), :] = weight_leaf[pl.ds(o, 1), pl.ds(128 * g, 128)]
    side = iota((64, 128), 1) < 64
    for e in range(2):
        each = []
        for o in range(STENCIL):
            part = lines[pl.ds(64 * o, 64), :]
            right = pltpu.roll(jnp.broadcast_to(part[:, e : e + 1], (64, 128)), 63, 0)
            left = pltpu.roll(jnp.broadcast_to(part[:, 126 + e : 127 + e], (64, 128)), 1, 0)
            each.append(jnp.where(side, right, left))
        for m in range(5):
            total = jnp.zeros((64, 128), F32)
            for o in range(STENCIL):
                total = total + jnp.where(offsets[o] == m - 2, each[o], 0.0)
            coef[2 * m + e] = total


def tables(phase_leaf, phase_low, weight_low, weight_leaf, offsets):
    return pl.pallas_call(
        table_kernel,
        out_shape=[
            jax.ShapeDtypeStruct((16, 1024), F32),
            jax.ShapeDtypeStruct((16, 1024), F32),
            jax.ShapeDtypeStruct((64, 512), F32),
            jax.ShapeDtypeStruct((64, 512), F32),
            jax.ShapeDtypeStruct((8, 256, 256), BF16),
            jax.ShapeDtypeStruct((10, 64, 128), F32),
        ],
        in_specs=[VMEM, VMEM, VMEM, VMEM, SMEM],
        out_specs=[VMEM] * 6,
        scratch_shapes=[pltpu.VMEM((256, 128), F32)],
        compiler_params=pltpu.CompilerParams(vmem_limit_bytes=16 * 2**20),
        name="tables",
    )(phase_leaf, phase_low, weight_low, weight_leaf, offsets)


def receive_kernel(
    got, leaf_cos, leaf_sin, low_cos, low_sin, low_weight, coef, out,
    flat, parts, low, result, sems,
):
    side = iota((64, 128), 1) < 64
    lane = iota((64, 128), 1)

    def line(i):
        return got[pl.ds(16 + i, 64, stride=ROWS), :]

    cs = line(4)

    def spread(right, left):
        right = pltpu.roll(jnp.broadcast_to(cs[:, right : right + 1], (64, 128)), 63, 0)
        left = pltpu.roll(jnp.broadcast_to(cs[:, left : left + 1], (64, 128)), 1, 0)
        return jnp.where(side, right, left)

    turned = []
    for e in range(2):
        t = line(2 + e)
        c = spread(e, 126 + e)
        s = spread(2 + e, 124 + e)
        is_x = (lane & 63) < 32
        other = jnp.where(is_x, pltpu.roll(t, 96, 1), pltpu.roll(t, 32, 1))
        turned.append(t * c + other * jnp.where(is_x, -s, s))
    e = [coef[2 * m] * turned[0] + coef[2 * m + 1] * turned[1] for m in range(5)]
    l0, l1 = line(0), line(1)
    e[1] = e[1] + jnp.where(side, 0.0, l0)
    e[2] = e[2] + jnp.where(side, l0, l1)
    e[3] = e[3] + jnp.where(side, l1, 0.0)

    def before(v):
        return pltpu.roll(v, 1, 0)

    def after(v):
        return pltpu.roll(v, 63, 0)

    def swap(v):
        return pltpu.roll(v, 64, 1)

    rows = {
        0: jnp.where(side, before(e[2]) + swap(e[3]), 0.0),
        1: jnp.where(side, before(e[3]) + swap(e[4]), 0.0),
        2: jnp.where(side, before(e[4]), 0.0),
        13: jnp.where(side, 0.0, after(e[0])),
        14: jnp.where(side, 0.0, after(e[1]) + swap(e[0])),
        15: jnp.where(side, 0.0, after(e[2]) + swap(e[1])),
    }
    for block in range(8):
        tiles = []
        for i in range(16):
            tile = got[pl.ds(8 * ROWS * block + i, 8, stride=ROWS), :]
            if i in rows:
                tile = tile + rows[i][8 * block : 8 * block + 8]
            tiles.append(tile)
        flat[block] = jnp.concatenate(tiles, axis=0).T

    def anterpolate(block, start, count):
        at = pl.ds(128 * block, 128)
        rows = []
        for child in range(8):
            pair = []
            for h in range(2):
                x = flat[block, pl.ds(64 * h + start, count), :]
                y = flat[block, pl.ds(64 * h + 32 + start, count), :]
                c = leaf_cos[pl.ds(8 * h + child, 1), at]
                s = leaf_sin[pl.ds(8 * h + child, 1), at]
                pair.append((x * c - y * s, x * s + y * c))
            for component in range(2):
                rows.append(jnp.concatenate([pair[0][component], pair[1][component]], axis=1))
        high, low = halves(jnp.concatenate(rows, axis=0))
        w = low_weight[block]
        y = product(high, w) + product(low, w)
        return y[:, :128] + y[:, 128:]

    wide = iota((16 * COUNT, 128), 1)

    def copy(c, t, start):
        here = (c, pl.ds(start, CHUNK), slice(None), pl.ds(128 * t, 128))
        return pltpu.make_async_copy(result.at[here], out.at[here], sems.at[c, t, start // CHUNK])

    def emit(start, t):
        def step(i, carry):
            for child in range(8):
                to = pl.ds(8 * child, 8), pl.ds(128 * t, 128)
                c, s = low_cos[to], low_sin[to]
                for k in range(PER):
                    r = PER * i + k
                    x = low[pl.ds(2 * COUNT * child + r, 1), :]
                    y = low[pl.ds(2 * COUNT * child + COUNT + r, 1), :]
                    result[(0, start + r) + to] = x * c - y * s
                    result[(1, start + r) + to] = x * s + y * c
            for k in range(PER // CHUNK):
                for c in range(2):
                    copy(c, t, start + PER * i + CHUNK * k).start()
            return carry

        for i in range(COUNT // PER):
            step(i, 0)

    for part in range(32 // COUNT):
        start = COUNT * part
        for t, blocks in enumerate(((7, 0, 1, 2), (3, 4), (5, 6), ())):
            for block in blocks:
                parts[block] = anterpolate(block, start, COUNT)
            here, there, after_, before_ = (parts[k % 8] for k in (2 * t, 2 * t + 1, 2 * t + 2, 2 * t + 7))
            low[...] = jnp.where(wide >= 126, after_, here) + jnp.where(wide < 2, before_, there)
            emit(start, t)

    for t in range(4):
        for k in range(32 // CHUNK):
            for c in range(2):
                copy(c, t, CHUNK * k).wait()


RECEIVE_SCRATCH = [
    pltpu.VMEM((8, 128, 128), F32),
    pltpu.VMEM((8, 16 * COUNT, 128), F32),
    pltpu.VMEM((16 * COUNT, 128), F32),
    pltpu.VMEM((2, 32, 64, 512), F32),
    pltpu.SemaphoreType.DMA((2, 4, 32 // CHUNK)),
]


def receive(got, ready):
    return pl.pallas_call(
        receive_kernel,
        out_shape=jax.ShapeDtypeStruct((2, 32, 64, 512), F32),
        in_specs=[VMEM] * 7,
        out_specs=HBM,
        scratch_shapes=RECEIVE_SCRATCH,
        compiler_params=pltpu.CompilerParams(vmem_limit_bytes=32 * 2**20),
        name="receive",
    )(got, *ready)


def body(
    incoming, own_field, phase_mid, phase_leaf, phase_low,
    weight_top, weight_leaf, weight_low, offsets, owner,
):
    incoming, own_field, phase_mid, phase_leaf, phase_low, weight_top, weight_leaf, weight_low, offsets, owner = (
        pltpu.with_memory_space_constraint(value, pltpu.HBM)
        for value in (
            incoming, own_field, phase_mid, phase_leaf, phase_low,
            weight_top, weight_leaf, weight_low, offsets, owner,
        )
    )
    message = send(incoming, own_field, phase_mid, weight_top, weight_leaf, offsets, owner)
    message = message.reshape(ANG, 1, ROWS * 128)
    got = lax.all_to_all(message, "ang", split_axis=0, concat_axis=0, tiled=True)
    got = got.reshape(ANG * ROWS, 128)
    ready = tables(phase_leaf, phase_low, weight_low, weight_leaf, offsets)
    return receive(got, ready)


def solution(mesh):
    placed = (
        P(None, None, "box", "ang"),
        P(None, None, "box", "ang"),
        P("box", "ang"),
        P(("ang", "box"), None),
        P(("ang", "box"), None),
        P(None, "ang"),
        P(),
        P(),
        P(),
        P(),
    )
    return jax.shard_map(
        body,
        mesh=mesh,
        in_specs=placed,
        out_specs=P(None, None, ("ang", "box"), None),
        check_vma=False,
    )
```

```python
import functools

import jax
import jax.numpy as jnp
from jax import lax
from jax.experimental import pallas as pl
from jax.experimental.pallas import tpu as pltpu
from jax.sharding import PartitionSpec as P

STENCIL = 4
ANG = 64
ROWS = 21
PITCH = 72
COUNT = 16
PER = 16
CHUNK = 16
ORDER = (
    53, 29, 32, 22, 39, 40, 28, 26, 50, 42, 49, 20, 55, 43, 58, 47,
    0, 57, 37, 2, 8, 15, 24, 31, 7, 38, 36, 21, 52, 60, 27, 56,
    45, 51, 62, 10, 12, 44, 41, 54, 13, 16, 61, 11, 17, 23, 34, 33,
    14, 3, 48, 18, 35, 59, 1, 4, 5, 9, 63, 25, 46, 6, 19, 30,
)
PLACE = tuple(ORDER.index(g) for g in range(ANG))
NT = (((1,), (1,)), ((), ()))
F32 = jnp.float32
BF16 = jnp.bfloat16
VMEM = pl.BlockSpec(memory_space=pltpu.VMEM)
SMEM = pl.BlockSpec(memory_space=pltpu.SMEM)
HBM = pl.BlockSpec(memory_space=pltpu.HBM)


def halves(value):
    high = value.astype(BF16)
    return high, (value - high.astype(F32)).astype(BF16)


def iota(shape, dim):
    return lax.broadcasted_iota(jnp.int32, shape, dim)


def turn(angle):
    count = jnp.floor(angle * 0.6366197723675814 + 0.5)
    rest = angle - count * 1.5703125
    rest = rest - count * 4.837512969970703e-4
    rest = rest - count * 7.549789954891e-8
    square = rest * rest
    sine = ((-1.9515295891e-4 * square + 8.3321608736e-3) * square - 1.6666654611e-1) * square * rest + rest
    cosine = ((2.443315711809948e-5 * square - 1.388731625493765e-3) * square + 4.166664568298827e-2) * square
    cosine = cosine * square - 0.5 * square + 1.0
    quarter = count.astype(jnp.int32)
    odd = (quarter & 1) == 1
    first = jnp.where(odd, sine, cosine)
    second = jnp.where(odd, cosine, sine)
    return (
        jnp.where(((quarter + 1) & 2) == 2, -first, first),
        jnp.where((quarter & 2) == 2, -second, second),
    )


def window(hits, weights):
    total = None
    for o in range(STENCIL):
        term = jnp.where(hits[o], weights[o], 0.0)
        total = term if total is None else total + term
    return halves(total)


def placed(piece, start):
    begin = (start - 8) % 128
    zero = jnp.zeros((80, 128), BF16)
    if begin + 48 <= 128:
        return jnp.concatenate([zero[:begin], piece, zero[begin:]], axis=0)
    over = begin + 48 - 128
    return jnp.concatenate([piece[48 - over :], zero, piece[: 48 - over]], axis=0)


def product(left, right):
    return lax.dot_general(left, right, NT, preferred_element_type=F32)


def send_kernel(
    incoming, own, all_phase, all_top, all_leaf, all_offsets, all_owner, message,
    fine, field, phase, weight_top, local, offsets, owner, place, spread_own, coarse, rims, sems,
):
    ang = lax.axis_index("ang")
    box = lax.axis_index("box")
    small = [
        pltpu.make_async_copy(source, target, sems.at[i])
        for i, (source, target) in enumerate(
            (
                (all_phase, phase),
                (all_offsets, offsets),
                (all_top, weight_top),
                (all_leaf.at[:, pl.ds(pl.multiple_of(ang * 128, 128), 128)], local),
                (all_owner, owner),
            )
        )
    ]
    get_fine = [
        pltpu.make_async_copy(incoming.at[i // 2, pl.ds(16 * (i % 2), 16)], fine.at[i], sems.at[5 + i])
        for i in range(4)
    ]
    get_field = [pltpu.make_async_copy(own.at[c], field.at[c], sems.at[9 + c]) for c in range(2)]
    for copy in small + get_fine + get_field:
        copy.start()

    for g in range(ANG):
        place[g] = PLACE[g]
    small[0].wait()
    cosine, sine = turn(phase[...])
    lane = iota((64, 128), 1)
    rim_phase = jnp.where(
        (lane < 2) | (lane >= 126),
        cosine,
        jnp.where(lane < 64, pltpu.roll(sine, 2, 1), pltpu.roll(sine, 126, 1)),
    )

    small[1].wait()
    small[2].wait()
    apart = iota((48, 128), 0) - 8 - iota((48, 128), 1) // 4
    hits = [apart == offsets[o] for o in range(STENCIL)]
    top = []
    for part in range(2):
        highs, lows = [], []
        for k in (2 * part, 2 * part + 1):
            high, low = window(hits, [weight_top[o : o + 1, 128 * k : 128 * k + 128] for o in range(STENCIL)])
            highs.append(placed(high, 32 * k))
            lows.append(placed(low, 32 * k))
        top.append(jnp.concatenate([jnp.concatenate(highs, axis=1), jnp.concatenate(lows, axis=1)], axis=0))

    row = iota((48, 128), 0)
    inner = row % 24
    first = row < 24
    at = jnp.where(inner < 16, inner + jnp.where(first, 0, 16), inner - 16 + jnp.where(first, 32, -2))
    at = jnp.where(inner < 18, at, -100)
    apart = at - iota((48, 128), 1) // 4
    small[3].wait()
    high, low = window(
        [apart == offsets[o] for o in range(STENCIL)], [local[o : o + 1, :] for o in range(STENCIL)]
    )
    leaf = jnp.concatenate(
        [jnp.concatenate([high, high], axis=1), jnp.concatenate([low, low], axis=1)], axis=0
    )

    wide = iota((128, 128), 1)
    for block in range(4):
        get_fine[block].wait()
        rows = fine[block].reshape(128, 512)
        high, low = halves(rows)
        sums = []
        for part in range(2):
            a = high[:, 256 * part : 256 * part + 256]
            b = low[:, 256 * part : 256 * part + 256]
            y = product(a, top[part]) + product(b, top[part])
            sums.append(y[:, :128] + y[:, 128:])
        coarse[pl.ds(128 * block, 128), :] = jnp.where(
            wide < 2, sums[0], jnp.where(wide >= 126, sums[1], sums[0] + sums[1])
        )
        rims[pl.ds(128 * block, 128), :] = jnp.where(wide >= 64, sums[0], sums[1])

    srow = iota((16, 128), 0)
    slane = iota((16, 128), 1)
    pick = (
        ((srow == 2) & (slane == 0))
        | ((srow == 3) & (slane == 1))
        | ((srow == 10) & (slane == 126))
        | ((srow == 11) & (slane == 127))
    )
    pick = jnp.where(pick, 1.0, 0.0).astype(BF16)
    pick = jnp.concatenate([pick, pick], axis=1)
    rim_tiles = []
    side = iota((8, 128), 1) < 64
    for pair in range(4):
        stacked = []
        for p in (2 * pair, 2 * pair + 1):
            for c in range(2):
                stacked.append(rims[pl.ds(c * 256 + p, 32, stride=8), :])
        high, low = halves(jnp.concatenate(stacked, axis=0))
        got = product(pick, jnp.concatenate([high, low], axis=1))
        right, left = got[:8], got[8:]
        rim_tiles.append(jnp.where(side, right, pltpu.roll(left, 64, 1)))
        rim_tiles.append(jnp.where(side, pltpu.roll(right, 64, 1), left))

    for c in range(2):
        get_field[c].wait()
        for r in range(32):
            spread_own[pl.ds((c * 32 + r) * PITCH, 64), :] = field[c, r].astype(F32)

    small[4].wait()
    half = iota((24, 128), 1) < 64
    fifth = iota((8, 128), 0) == 4
    for p in range(8):
        x = coarse[pl.ds(p, 32, stride=8), :]
        y = coarse[pl.ds(256 + p, 32, stride=8), :]
        for quad in range(2):
            highs, lows = [], []
            for child in range(4):
                b = 8 * p + 4 * quad + child
                c = cosine[b : b + 1]
                s = sine[b : b + 1]
                ox = spread_own[pl.ds(b, 32, stride=PITCH), :]
                oy = spread_own[pl.ds(32 * PITCH + b, 32, stride=PITCH), :]
                for z in (x * c - y * s + ox, x * s + y * c + oy):
                    high, low = halves(z)
                    highs.append(high)
                    lows.append(low)
            right = jnp.concatenate(
                [jnp.concatenate(highs, axis=0), jnp.concatenate(lows, axis=0)], axis=1
            )
            got = product(leaf, right)
            got = got[:48] + got[48:]
            for pair in range(2):
                a = got[:24, 128 * pair : 128 * pair + 128]
                d = got[24:, 128 * pair : 128 * pair + 128]
                for odd in range(2):
                    b = 8 * p + 4 * quad + 2 * pair + odd
                    if odd:
                        tile = jnp.where(half, pltpu.roll(a, 64, 1), d)
                    else:
                        tile = jnp.where(half, a, pltpu.roll(d, 64, 1))
                    target = place[owner[box, b]] * ROWS
                    extra = rim_tiles[p] + jnp.where(fifth, rim_phase[b : b + 1], 0.0)
                    message[pl.ds(target, 16), :] = tile[:16]
                    message[pl.ds(target + 16, 5), :] = (tile[16:] + extra)[:5]


def send(incoming, own, phase, weight_top, weight_leaf, offsets, owner):
    return pl.pallas_call(
        send_kernel,
        out_shape=jax.ShapeDtypeStruct((ANG * ROWS, 128), F32),
        in_specs=[HBM] * 7,
        out_specs=VMEM,
        scratch_shapes=SEND_SCRATCH,
        compiler_params=pltpu.CompilerParams(vmem_limit_bytes=24 * 2**20),
        name="send",
    )(incoming, own, phase, weight_top, weight_leaf, offsets, owner)


SEND_SCRATCH = [
    pltpu.VMEM((4, 16, 8, 512), F32),
    pltpu.VMEM((2, 32, 64, 128), BF16),
    pltpu.VMEM((64, 128), F32),
    pltpu.VMEM((4, 512), F32),
    pltpu.VMEM((4, 128), F32),
    pltpu.SMEM((4,), jnp.int32),
    pltpu.SMEM((4, 64), jnp.int32),
    pltpu.SMEM((64,), jnp.int32),
    pltpu.VMEM((64 * PITCH, 128), F32),
    pltpu.VMEM((512, 128), F32),
    pltpu.VMEM((512, 128), F32),
    pltpu.SemaphoreType.DMA((11,)),
]


def table_kernel(
    phase_leaf, phase_low, weight_low, weight_leaf, offsets,
    leaf_cos, leaf_sin, low_cos, low_sin, low_weight, coef, lines,
):
    low_cos[...], low_sin[...] = turn(phase_low[...])
    row, column = iota((256, 256), 0), iota((256, 256), 1)
    order = jnp.where(column == (row % 8) * 32 + (row // 128) * 16 + (row % 128) // 8, 1.0, 0.0).astype(BF16)
    stacked = []
    for block in range(8):
        stacked.append(phase_leaf[:, 256 * block : 256 * block + 256])
        stacked.append(weight_low[:, 256 * block : 256 * block + 256])
        stacked.append(weight_low[:, 256 * block : 256 * block + 256])
    stacked = jnp.concatenate(stacked, axis=0)
    high, rest = stacked.astype(BF16), stacked
    rest = rest - high.astype(F32)
    middle = rest.astype(BF16)
    low = (rest - middle.astype(F32)).astype(BF16)
    sorted_ = product(high, order) + product(middle, order) + product(low, order)
    at, lane = iota((128, 128), 0), iota((128, 128), 1)
    for block in range(8):
        columns = []
        for h in range(2):
            part = sorted_[16 * block : 16 * block + 16, 128 * h : 128 * h + 128]
            to = pl.ds(128 * block, 128)
            leaf_cos[pl.ds(8 * h, 8), to], leaf_sin[pl.ds(8 * h, 8), to] = turn(part[:8])
            apart = (at - (64 * block + (lane % 8) * 8 + 4 * h + lane // 32)) & 127
            hits = [apart == (offsets[o] & 127) for o in range(STENCIL)]
            columns.append(jnp.concatenate(window(hits, [part[8 + o : 9 + o] for o in range(STENCIL)]), axis=0))
        low_weight[block] = jnp.concatenate(columns, axis=1)

    for o in range(STENCIL):
        for g in range(ANG):
            lines[pl.ds(64 * o + g, 1), :] = weight_leaf[pl.ds(o, 1), pl.ds(128 * g, 128)]
    side = iota((64, 128), 1) < 64
    for e in range(2):
        each = []
        for o in range(STENCIL):
            part = lines[pl.ds(64 * o, 64), :]
            right = pltpu.roll(jnp.broadcast_to(part[:, e : e + 1], (64, 128)), 63, 0)
            left = pltpu.roll(jnp.broadcast_to(part[:, 126 + e : 127 + e], (64, 128)), 1, 0)
            each.append(jnp.where(side, right, left))
        for m in range(5):
            total = jnp.zeros((64, 128), F32)
            for o in range(STENCIL):
                total = total + jnp.where(offsets[o] == m - 2, each[o], 0.0)
            coef[2 * m + e] = total


def tables(phase_leaf, phase_low, weight_low, weight_leaf, offsets):
    return pl.pallas_call(
        table_kernel,
        out_shape=[
            jax.ShapeDtypeStruct((16, 1024), F32),
            jax.ShapeDtypeStruct((16, 1024), F32),
            jax.ShapeDtypeStruct((64, 512), F32),
            jax.ShapeDtypeStruct((64, 512), F32),
            jax.ShapeDtypeStruct((8, 256, 256), BF16),
            jax.ShapeDtypeStruct((10, 64, 128), F32),
        ],
        in_specs=[VMEM, VMEM, VMEM, VMEM, SMEM],
        out_specs=[VMEM] * 6,
        scratch_shapes=[pltpu.VMEM((256, 128), F32)],
        compiler_params=pltpu.CompilerParams(vmem_limit_bytes=16 * 2**20),
        name="tables",
    )(phase_leaf, phase_low, weight_low, weight_leaf, offsets)


def receive_kernel(
    got, leaf_cos, leaf_sin, low_cos, low_sin, low_weight, coef, out,
    flat, parts, low, result, sems,
):
    side = iota((64, 128), 1) < 64
    lane = iota((64, 128), 1)

    def rows_of(sources, i):
        return jnp.concatenate([got[pl.ds(ROWS * PLACE[g] + i, 1), :] for g in sources], axis=0)

    def line(i):
        return rows_of(range(ANG), 16 + i)

    cs = line(4)

    def spread(right, left):
        right = pltpu.roll(jnp.broadcast_to(cs[:, right : right + 1], (64, 128)), 63, 0)
        left = pltpu.roll(jnp.broadcast_to(cs[:, left : left + 1], (64, 128)), 1, 0)
        return jnp.where(side, right, left)

    turned = []
    for e in range(2):
        t = line(2 + e)
        c = spread(e, 126 + e)
        s = spread(2 + e, 124 + e)
        is_x = (lane & 63) < 32
        other = jnp.where(is_x, pltpu.roll(t, 96, 1), pltpu.roll(t, 32, 1))
        turned.append(t * c + other * jnp.where(is_x, -s, s))
    e = [coef[2 * m] * turned[0] + coef[2 * m + 1] * turned[1] for m in range(5)]
    l0, l1 = line(0), line(1)
    e[1] = e[1] + jnp.where(side, 0.0, l0)
    e[2] = e[2] + jnp.where(side, l0, l1)
    e[3] = e[3] + jnp.where(side, l1, 0.0)

    def before(v):
        return pltpu.roll(v, 1, 0)

    def after(v):
        return pltpu.roll(v, 63, 0)

    def swap(v):
        return pltpu.roll(v, 64, 1)

    rows = {
        0: jnp.where(side, before(e[2]) + swap(e[3]), 0.0),
        1: jnp.where(side, before(e[3]) + swap(e[4]), 0.0),
        2: jnp.where(side, before(e[4]), 0.0),
        13: jnp.where(side, 0.0, after(e[0])),
        14: jnp.where(side, 0.0, after(e[1]) + swap(e[0])),
        15: jnp.where(side, 0.0, after(e[2]) + swap(e[1])),
    }
    for block in range(8):
        tiles = []
        for i in range(16):
            tile = rows_of(range(8 * block, 8 * block + 8), i)
            if i in rows:
                tile = tile + rows[i][8 * block : 8 * block + 8]
            tiles.append(tile)
        flat[block] = jnp.concatenate(tiles, axis=0).T

    def anterpolate(block, start, count):
        at = pl.ds(128 * block, 128)
        rows = []
        for child in range(8):
            pair = []
            for h in range(2):
                x = flat[block, pl.ds(64 * h + start, count), :]
                y = flat[block, pl.ds(64 * h + 32 + start, count), :]
                c = leaf_cos[pl.ds(8 * h + child, 1), at]
                s = leaf_sin[pl.ds(8 * h + child, 1), at]
                pair.append((x * c - y * s, x * s + y * c))
            for component in range(2):
                rows.append(jnp.concatenate([pair[0][component], pair[1][component]], axis=1))
        high, low = halves(jnp.concatenate(rows, axis=0))
        w = low_weight[block]
        y = product(high, w) + product(low, w)
        return y[:, :128] + y[:, 128:]

    wide = iota((16 * COUNT, 128), 1)

    def copy(c, t, start):
        here = (c, pl.ds(start, CHUNK), slice(None), pl.ds(128 * t, 128))
        return pltpu.make_async_copy(result.at[here], out.at[here], sems.at[c, t, start // CHUNK])

    def emit(start, t):
        def step(i, carry):
            for child in range(8):
                to = pl.ds(8 * child, 8), pl.ds(128 * t, 128)
                c, s = low_cos[to], low_sin[to]
                for k in range(PER):
                    r = PER * i + k
                    x = low[pl.ds(2 * COUNT * child + r, 1), :]
                    y = low[pl.ds(2 * COUNT * child + COUNT + r, 1), :]
                    result[(0, start + r) + to] = x * c - y * s
                    result[(1, start + r) + to] = x * s + y * c
            for k in range(PER // CHUNK):
                for c in range(2):
                    copy(c, t, start + PER * i + CHUNK * k).start()
            return carry

        for i in range(COUNT // PER):
            step(i, 0)

    for part in range(32 // COUNT):
        start = COUNT * part
        for t, blocks in enumerate(((7, 0, 1, 2), (3, 4), (5, 6), ())):
            for block in blocks:
                parts[block] = anterpolate(block, start, COUNT)
            here, there, after_, before_ = (parts[k % 8] for k in (2 * t, 2 * t + 1, 2 * t + 2, 2 * t + 7))
            low[...] = jnp.where(wide >= 126, after_, here) + jnp.where(wide < 2, before_, there)
            emit(start, t)

    for t in range(4):
        for k in range(32 // CHUNK):
            for c in range(2):
                copy(c, t, CHUNK * k).wait()


RECEIVE_SCRATCH = [
    pltpu.VMEM((8, 128, 128), F32),
    pltpu.VMEM((8, 16 * COUNT, 128), F32),
    pltpu.VMEM((16 * COUNT, 128), F32),
    pltpu.VMEM((2, 32, 64, 512), F32),
    pltpu.SemaphoreType.DMA((2, 4, 32 // CHUNK)),
]


def receive(got, ready):
    return pl.pallas_call(
        receive_kernel,
        out_shape=jax.ShapeDtypeStruct((2, 32, 64, 512), F32),
        in_specs=[VMEM] * 7,
        out_specs=HBM,
        scratch_shapes=RECEIVE_SCRATCH,
        compiler_params=pltpu.CompilerParams(vmem_limit_bytes=32 * 2**20),
        name="receive",
    )(got, *ready)


def body(
    incoming, own_field, phase_mid, phase_leaf, phase_low,
    weight_top, weight_leaf, weight_low, offsets, owner,
):
    incoming, own_field, phase_mid, phase_leaf, phase_low, weight_top, weight_leaf, weight_low, offsets, owner = (
        pltpu.with_memory_space_constraint(value, pltpu.HBM)
        for value in (
            incoming, own_field, phase_mid, phase_leaf, phase_low,
            weight_top, weight_leaf, weight_low, offsets, owner,
        )
    )
    message = send(incoming, own_field, phase_mid, weight_top, weight_leaf, offsets, owner)
    message = message.reshape(ANG, 1, ROWS * 128)
    got = lax.all_to_all(message, "ang", split_axis=0, concat_axis=0, tiled=True, axis_index_groups=[list(ORDER)])
    got = got.reshape(ANG * ROWS, 128)
    ready = tables(phase_leaf, phase_low, weight_low, weight_leaf, offsets)
    return receive(got, ready)


def solution(mesh):
    placed = (
        P(None, None, "box", "ang"),
        P(None, None, "box", "ang"),
        P("box", "ang"),
        P(("ang", "box"), None),
        P(("ang", "box"), None),
        P(None, "ang"),
        P(),
        P(),
        P(),
        P(),
    )
    return jax.shard_map(
        body,
        mesh=mesh,
        in_specs=placed,
        out_specs=P(None, None, ("ang", "box"), None),
        check_vma=False,
    )
```
